32 devices in a mesh: lat: 16 (over z, y, core), lon: 2 (over x).
Axes of the slice: x: 2, y: 2, z: 4, core: 2. Of those that a mesh axis runs over, the one named last changes fastest.
Arguments:
- eastward_speed_face: float32 [72, 512, 256], P(None, 'lat', 'lon'), may hold values from -6 to 6
- northward_speed_face: float32 [72, 512, 256], P(None, 'lat', 'lon'), may hold values from -6 to 6
- stratum_extent_east_face: float32 [72, 512, 256], P(None, 'lat', 'lon'), may hold values from 0.5 to 2
- stratum_extent_north_face: float32 [72, 512, 256], P(None, 'lat', 'lon'), may hold values from 0.5 to 2
- northward_span_east_face: float32 [512, 256], P('lat', 'lon'), may hold values from 0.5 to 2
- eastward_span_north_face: float32 [512, 256], P('lat', 'lon'), may hold values from 0.5 to 2
- ocean_flag_east_face: int32 [72, 512, 256], P(None, 'lat', 'lon'), may hold values 0 or 1
- ocean_flag_north_face: int32 [72, 512, 256], P(None, 'lat', 'lon'), may hold values 0 or 1
- counterpart_across_seam: int32 [256], replicated, may hold values from 0 to 255, as said below
Outputs:
- eastward_speed_next: float32 [72, 512, 256], P(None, 'lat', 'lon')
- northward_speed_next: float32 [72, 512, 256], P(None, 'lat', 'lon')
The draws below stay inside these ranges and needn't reach their ends.
Inputs may be any that keep to these rules, and one draw needn't show every extreme that they name: counterpart_across_seam[i] = (p - 1 - i) mod 256 for one pivot p drawn anew in each draw; it is its own inverse.
All inputs are finite; a program needn't handle non-finite values. No bound on the sum of `ocean_flag_east_face` or of `ocean_flag_north_face` on one device may be relied on, other than what follows from the above.
Results may differ from the reference program's by a relative error of at most 0.00002.
Values sent between devices are 32-bit elements; how exact they have to be, the bound alone decides.
No kernel may reach another device: no remote copies, remote signals or barrier semaphores. Data moves between devices by JAX's collectives and lax.ppermute only.
A program may use at most 128 MiB of HBM per device.

```python
import math
import jax
import jax.numpy as jnp
from jax import lax

STRATA_COUNT = 72
NORTHWARD_CELLS = 512
EASTWARD_CELLS = 256


def draw_counterpart_across_seam(key, part):
    pivot = jax.random.randint(jax.random.fold_in(key, 17), (), 0, EASTWARD_CELLS)
    columns = jnp.arange(EASTWARD_CELLS, dtype=jnp.int32)
    return ((pivot - 1 - columns) % EASTWARD_CELLS).astype(jnp.int32)


def touch_ends(values, rng, low, high):
    longest = values.shape.index(max(values.shape))
    spots = []
    for shift in (0, 1):
        where = [jax.random.randint(jax.random.fold_in(rng, axis), (), 0, length) for axis, length in enumerate(values.shape)]
        where[longest] = (where[longest] + shift) % values.shape[longest]
        spots.append(tuple(where))
    return values.at[spots[0]].set(low).at[spots[1]].set(high)


def shard_levels(rng, shape, pieces, least, top_value):
    def one(dim, parts):
        draws = jax.random.uniform(jax.random.fold_in(jax.random.fold_in(rng, 6), dim), (parts,), jnp.float32, least / len(pieces), top_value / len(pieces))
        return jnp.repeat(jnp.exp(draws), shape[dim] // parts).reshape((-1,) + (1,) * (len(shape) - dim - 1))

    loudness = one(*pieces[0])
    for cut in pieces[1:]:
        loudness = loudness * one(*cut)
    return loudness


def centred(key, shape, scale, most, pieces=(), kind=jnp.bfloat16):
    loudness = shard_levels(key, shape, pieces, -0.22, 0.18) if pieces else 1.0
    values = jax.random.normal(key, shape, jnp.float32) * scale * loudness
    return jnp.minimum(jnp.maximum(values, -most), most).astype(kind)


def setup_inputs(seed: int = 0) -> dict:
    key_of = jax.random.split(jax.random.key(seed), 10)
    return {
        "eastward_speed_face": centred(key_of[0], (STRATA_COUNT, NORTHWARD_CELLS, EASTWARD_CELLS), 1.0, 6.0, ((1, 16), (2, 2)), jnp.float32),
        "northward_speed_face": centred(key_of[1], (STRATA_COUNT, NORTHWARD_CELLS, EASTWARD_CELLS), 1.0, 6.0, ((1, 16), (2, 2)), jnp.float32),
        "stratum_extent_east_face": jnp.clip(jnp.exp(math.log(2.0) - 1.3862944 * jax.random.uniform(key_of[2], (STRATA_COUNT, NORTHWARD_CELLS, EASTWARD_CELLS), jnp.float32) ** shard_levels(key_of[2], (STRATA_COUNT, NORTHWARD_CELLS, EASTWARD_CELLS), ((1, 16), (2, 2)), -0.2, 0.2)), 0.5, 2.0),
        "stratum_extent_north_face": jnp.clip(jnp.exp(math.log(2.0) - 1.3862944 * jax.random.uniform(key_of[3], (STRATA_COUNT, NORTHWARD_CELLS, EASTWARD_CELLS), jnp.float32) ** shard_levels(key_of[3], (STRATA_COUNT, NORTHWARD_CELLS, EASTWARD_CELLS), ((1, 16), (2, 2)), -0.2, 0.2)), 0.5, 2.0),
        "northward_span_east_face": jnp.clip(jnp.exp(math.log(2.0) - 1.3862944 * jax.random.uniform(key_of[4], (NORTHWARD_CELLS, EASTWARD_CELLS), jnp.float32) ** shard_levels(key_of[4], (NORTHWARD_CELLS, EASTWARD_CELLS), ((0, 16), (1, 2)), -0.2, 0.2)), 0.5, 2.0),
        "eastward_span_north_face": jnp.clip(jnp.exp(math.log(2.0) - 1.3862944 * jax.random.uniform(key_of[5], (NORTHWARD_CELLS, EASTWARD_CELLS), jnp.float32) ** shard_levels(key_of[5], (NORTHWARD_CELLS, EASTWARD_CELLS), ((0, 16), (1, 2)), -0.2, 0.2)), 0.5, 2.0),
        "ocean_flag_east_face": touch_ends((jax.random.randint(key_of[6], (STRATA_COUNT, NORTHWARD_CELLS, EASTWARD_CELLS), 0, 4) < 3).astype(jnp.int32), jax.random.fold_in(key_of[6], 1), 0, 1),
        "ocean_flag_north_face": touch_ends((jax.random.randint(key_of[7], (STRATA_COUNT, NORTHWARD_CELLS, EASTWARD_CELLS), 0, 4) < 3).astype(jnp.int32), jax.random.fold_in(key_of[7], 1), 0, 1),
        "counterpart_across_seam": draw_counterpart_across_seam(jax.random.fold_in(key_of[9], 71), 0),
    }


time_step = 0.2


def interp(a, b, c, d):
    return (7.0 * (b + c) - (a + d)) / 12.0


def advect(umv, vmv, tuv, tvv, rows, cols):
    def cx(field, ro, co):
        return field[..., ro:ro + rows, co:co + cols + 1]

    def ry(field, ro, co):
        return field[..., ro:ro + rows + 1, co:co + cols]

    fut = 0.5 * (cx(tuv, 2, 1) + cx(tuv, 2, 2)) * interp(cx(umv, 2, 0), cx(umv, 2, 1), cx(umv, 2, 2), cx(umv, 2, 3))
    vface = ry(tvv, 1, 2)
    fvf = 0.5 * (vface + ry(tvv, 1, 3)) * interp(ry(umv, 0, 2), ry(umv, 1, 2), ry(umv, 2, 2), ry(umv, 3, 2))
    fuf = 0.5 * (cx(tuv, 2, 1) + cx(tuv, 3, 1)) * interp(cx(vmv, 2, 0), cx(vmv, 2, 1), cx(vmv, 2, 2), cx(vmv, 2, 3))
    fvt = 0.5 * (vface + ry(tvv, 2, 2)) * interp(ry(vmv, 0, 2), ry(vmv, 1, 2), ry(vmv, 2, 2), ry(vmv, 3, 2))
    trend_u = -((fut[..., 1:] - fut[..., :-1]) + (fvf[..., 1:, :] - fvf[..., :-1, :]))
    trend_v = -((fuf[..., 1:] - fuf[..., :-1]) + (fvt[..., 1:, :] - fvt[..., :-1, :]))
    return trend_u, trend_v


def extend(field, counterpart_across_seam):
    north = -field[-2:, :][::-1, :][:, counterpart_across_seam]
    south = jnp.zeros((2, field.shape[1]), jnp.float32)
    padded = jnp.concatenate([south, field, north], axis=0)
    return jnp.concatenate([padded[:, -2:], padded, padded[:, :2]], axis=1)


def reference(eastward_speed_face, northward_speed_face, stratum_extent_east_face, stratum_extent_north_face, northward_span_east_face, eastward_span_north_face, ocean_flag_east_face, ocean_flag_north_face, counterpart_across_seam):
    def stratum_index(items):
        uk, vk, e3uk, e3vk, umk, vmk = items
        um = umk.astype(jnp.float32) * uk
        vm = vmk.astype(jnp.float32) * vk
        volu = northward_span_east_face * e3uk
        volv = eastward_span_north_face * e3vk
        tu = volu * um
        tv = volv * vm
        ext = [extend(f, counterpart_across_seam) for f in (um, vm, tu, tv)]
        trend_u, trend_v = advect(ext[0], ext[1], ext[2], ext[3], um.shape[0], um.shape[1])
        u_new = umk.astype(jnp.float32) * (um + time_step * trend_u / volu)
        v_new = vmk.astype(jnp.float32) * (vm + time_step * trend_v / volv)
        return u_new, v_new

    eastward_speed_next, northward_speed_next = lax.map(stratum_index, (eastward_speed_face, northward_speed_face, stratum_extent_east_face, stratum_extent_north_face, ocean_flag_east_face, ocean_flag_north_face))
    return eastward_speed_next, northward_speed_next
```

```python
import functools

import jax
import jax.numpy as jnp
from jax import lax
from jax.experimental import pallas as pl
from jax.experimental.pallas import tpu as pltpu
from jax.sharding import PartitionSpec as P


time_step = 0.2
factor = -time_step / 24.0

LANES = 128
SUB = 8
SLOT = 16
DEPTH = 6
PAD = 8


def lane_ids():
    return lax.broadcasted_iota(jnp.int32, (SUB, LANES), 1)


def row_ids():
    return lax.broadcasted_iota(jnp.int32, (SUB, LANES), 0)


def right(x, shift):
    return pltpu.roll(x, shift % LANES, 1)


def strip_slots():
    return lax.rem(lane_ids(), SLOT)


def pack_kernel(
    levels, rows, lons,
    u_hbm, v_hbm, eu_hbm, ev_hbm, su_hbm, sv_hbm, fu_hbm, fv_hbm, seam_hbm,
    um, vm, tu, tv, ru, rv, strip_um, strip_vm, strip_tu, strip_tv,
    msg_a, msg_b, msg_x, msg_c, msg_d, source,
    u, v, eu, ev, fu, fv, su, sv, seam, sems, small_sems,
):
    pitch = rows + PAD
    groups = rows // SUB
    chunks = levels // SUB
    pairs = ((u_hbm, u), (v_hbm, v), (eu_hbm, eu), (ev_hbm, ev), (fu_hbm, fu), (fv_hbm, fv))
    strips = (strip_um, strip_vm, strip_tu, strip_tv)

    def big_copy(c, n):
        part = pl.ds(c * SUB, SUB)
        return pltpu.make_async_copy(pairs[n][0].at[part], pairs[n][1].at[part], sems.at[c, n])

    small = (
        pltpu.make_async_copy(su_hbm, su, small_sems.at[0]),
        pltpu.make_async_copy(sv_hbm, sv, small_sems.at[1]),
        pltpu.make_async_copy(seam_hbm, seam, small_sems.at[2]),
    )
    small[0].start()
    small[1].start()
    for c in range(chunks):
        for n in range(6):
            big_copy(c, n).start()
    small[2].start()
    small[0].wait()
    small[1].wait()

    lane = lane_ids()
    slot = strip_slots()

    def chunk(c, carry):
        for n in range(6):
            big_copy(c, n).wait()
        spans = [(su[pl.ds(g * SUB, SUB), :], sv[pl.ds(g * SUB, SUB), :]) for g in range(groups)]

        def first(g, s):
            k = c * SUB + s
            part = pl.ds(g * SUB, SUB)
            own = pl.ds(k * pitch + PAD + g * SUB, SUB)
            flat = pl.ds(k * rows + g * SUB, SUB)
            flag_u = fu[k, part, :].astype(jnp.float32)
            flag_v = fv[k, part, :].astype(jnp.float32)
            mu = flag_u * u[k, part, :]
            mv = flag_v * v[k, part, :]
            vol_u = spans[g][0] * eu[k, part, :]
            vol_v = spans[g][1] * ev[k, part, :]
            fields = (mu, mv, vol_u * mu, vol_v * mv)
            moved = []
            for field in fields:
                moved.append((right(field, SLOT * s + 4), right(field, SLOT * s + 8)))
            for ref, field in zip((um, vm, tu, tv), fields):
                ref[own, :] = field
            ru[flat, :] = flag_u * (factor / vol_u)
            rv[flat, :] = flag_v * (factor / vol_v)
            return moved

        sums = [None] * 4

        def second(g, s, moved):
            for n in range(4):
                east, west = moved[n]
                sums[n] = east if s == 0 else jnp.where(lane >= SLOT * s, east, sums[n])
                sums[n] = jnp.where(lane >= SLOT * s + 8, west, sums[n])
            if s == SUB - 1:
                for n in range(4):
                    strips[n][pl.ds(c * pitch + PAD + g * SUB, SUB), :] = sums[n]

        units = [(g, s) for g in range(groups) for s in range(SUB)]
        held = []
        for i in range(len(units) + DEPTH):
            if i < len(units):
                held.append(first(*units[i]))
            if i >= DEPTH:
                second(*units[i - DEPTH], held[i - DEPTH])
        shifted = []
        for g in range(groups):
            values = [ref[pl.ds(c * pitch + PAD + g * SUB, SUB), :] for ref in strips]
            shifted.append([(right(x, 4 * n - 8), right(x, 4 * n)) for n, x in enumerate(values)])
        for g in range(groups):
            packed = shifted[g][0][0]
            for n in range(4):
                if n:
                    packed = jnp.where(slot >= 4 * n, shifted[g][n][0], packed)
                packed = jnp.where(slot >= 4 * n + 2, shifted[g][n][1], packed)
            msg_x[c * groups + g] = packed
        return carry

    lax.fori_loop(0, chunks, chunk, 0)

    def row_of(ref, row):
        return ref[pl.ds(PAD + row, levels, stride=pitch), :]

    def pack_rows(ref, top):
        if top:
            picks = ((um, rows - 2), (um, rows - 1), (vm, rows - 2), (vm, rows - 1), (tu, rows - 1), (tv, rows - 1))
        else:
            picks = ((um, 0), (um, 1), (vm, 0), (vm, 1), (tu, 0), (tv, 0))
        for n, (field, row) in enumerate(picks):
            ref[n] = row_of(field, row)

    def pack_corner(ref, top):
        line = row_of(tv, rows - 1) if top else row_of(tu, 0)
        moved = [right(line[g * SUB : (g + 1) * SUB, :], g if top else g + 1) for g in range(chunks)]
        packed = moved[0]
        for g in range(1, chunks):
            packed = jnp.where(lane == g, moved[g], packed)
        ref[...] = packed

    odd = lax.rem(lax.axis_index("lat"), 2)

    @pl.when(odd == 0)
    def _():
        pack_corner(msg_c, True)
        pack_corner(msg_d, False)
        pack_rows(msg_a, True)
        pack_rows(msg_b, False)

    @pl.when(odd == 1)
    def _():
        pack_corner(msg_c, False)
        pack_corner(msg_d, True)
        pack_rows(msg_a, False)
        pack_rows(msg_b, True)

    small[2].wait()
    ring = lons * LANES
    where = seam[0] - lax.axis_index("lon") * LANES - lane
    source[...] = jnp.where(where < 0, where + ring, where)


def shifts(load):
    mu = [load(0, d) for d in range(-2, 3)]
    mv = [load(1, d) for d in range(-2, 3)]
    t0 = load(2, 0)
    both = t0 + load(2, 1)
    c0 = load(3, 0)
    below = load(3, -1)
    moved_u = [right(mu[2], d) for d in (1, 2, -1, -2)]
    moved_v = [right(mv[2], d) for d in (1, 2, -1, -2)]
    sides = (right(t0, 1), right(t0, -1), right(both, 1), right(c0, -1), right(below, -1))
    return mu, mv, t0, both, c0, below, load(3, 1), moved_u, moved_v, sides


def weigh(near, wide):
    return 7.0 * near - wide


def trends(held):
    mu, mv, t0, both, c0, below, above, moved_u, moved_v, sides = held
    left, after, both_left, c_east, below_east = sides
    m1, m2, p1, p2 = moved_u
    dx = (t0 + after) * weigh(mu[2] + p1, m1 + p2) - (left + t0) * weigh(m1 + mu[2], m2 + p1)
    dy = (c0 + c_east) * weigh(mu[2] + mu[3], mu[1] + mu[4])
    dy = dy - (below + below_east) * weigh(mu[1] + mu[2], mu[0] + mu[3])
    m1, m2, p1, p2 = moved_v
    ex = both * weigh(mv[2] + p1, m1 + p2) - both_left * weigh(m1 + mv[2], m2 + p1)
    ey = (c0 + above) * weigh(mv[2] + mv[3], mv[1] + mv[4])
    ey = ey - (below + c0) * weigh(mv[1] + mv[2], mv[0] + mv[3])
    return dx + dy, ex + ey


def pipelined(units, load, finish):
    held = []
    for i in range(len(units) + DEPTH):
        if i < len(units):
            held.append(shifts(load(*units[i])))
        if i >= DEPTH:
            finish(*units[i - DEPTH], held[i - DEPTH])
            held[i - DEPTH] = None


def inner_kernel(levels, rows, um, vm, tu, tv, ru, rv, u, v):
    pitch = rows + PAD
    groups = rows // SUB
    fields = (um, vm, tu, tv)

    def chunk(c, carry):
        def load(s, g):
            base = (c * SUB + s) * pitch + PAD + g * SUB
            return lambda n, d: fields[n][pl.ds(base + d, SUB), :]

        def finish(s, g, held):
            part = pl.ds((c * SUB + s) * rows + g * SUB, SUB)
            trend_u, trend_v = trends(held)
            u[part, :] = held[0][2] + ru[part, :] * trend_u
            v[part, :] = held[1][2] + rv[part, :] * trend_v

        pipelined([(s, g) for s in range(SUB) for g in range(groups)], load, finish)
        return carry

    lax.fori_loop(0, levels // SUB, chunk, 0)


def edge_kernel(
    levels, rows, lons, tops,
    um_in, vm_in, tu_in, tv_in, strip_um_in, strip_vm_in, strip_tu_in, strip_tv_in, u_in, v_in,
    ru, rv, got_a, got_b, bands, west_x, east_x, got_c, got_d, source,
    um, vm, tu, tv, strip_um, strip_vm, strip_tu, strip_tv, u, v, u_hbm, v_hbm,
    south, north, corners, trend_u, trend_v, sems,
):
    pitch = rows + PAD
    groups = rows // SUB
    chunks = levels // SUB
    lane = lane_ids()
    sub = row_ids()
    slot = strip_slots()
    mine = lax.div(lane, SLOT) == sub
    at = lax.axis_index("lat")
    odd = lax.rem(at, 2)
    is_top = at == tops - 1
    fields = (um, vm, tu, tv)
    strips = (strip_um, strip_vm, strip_tu, strip_tv)

    def pick(x, index):
        return jnp.take_along_axis(x, index, axis=1, mode="promise_in_bounds")

    @pl.when(odd == 0)
    def _():
        keep = at > 0
        for n in range(6):
            south[n] = jnp.where(keep, got_b[n], 0.0)
            north[n] = got_a[n]
        corners[0] = jnp.where(keep, got_d[...], 0.0)
        corners[1] = got_c[...]

    @pl.when(odd == 1)
    def _():
        for n in range(6):
            south[n] = got_a[n]
        corners[0] = got_c[...]

    @pl.when(jnp.logical_and(odd == 1, jnp.logical_not(is_top)))
    def _():
        for n in range(6):
            north[n] = got_b[n]
        corners[1] = got_d[...]

    @pl.when(is_top)
    def _():
        here = source[...]
        ring = lons * LANES
        before = jnp.where(here + 1 >= ring, 0, here + 1)
        column = lax.axis_index("lon")

        def mirrored(row, part, spot):
            within = lax.rem(spot, LANES)
            tile = lax.div(spot, LANES)
            out = jnp.zeros((SUB, LANES), jnp.float32)
            if lons == 2:
                sheets = ((column, bands[row, part, :]), (1 - column, got_b[row, part, :]))
            else:
                sheets = tuple((t, bands[t * 6 + row, part, :]) for t in range(lons))
            for t, sheet in sheets:
                out = jnp.where(tile == t, pick(sheet, within), out)
            return -out

        packed = jnp.zeros((SUB, LANES), jnp.float32)
        for g in range(chunks):
            part = pl.ds(g * SUB, SUB)
            for n, row in enumerate((1, 0, 3, 2, 4, 5)):
                north[n, part, :] = mirrored(row, part, here)
            packed = jnp.where(lane == g, right(mirrored(4, part, before), g), packed)
        corners[1] = packed

    from_west = lax.rem(lane, 4) >= 2
    halo_lanes = (slot >= 4) & (slot < 8)

    def incoming(c):
        out = []
        for g in range(groups):
            got = west_x[c * groups + g]
            if lons > 2:
                got = jnp.where(from_west, got, east_x[c * groups + g])
            out.append([right(got, 4 - 4 * n) for n in range(4)])
        return out

    def insert(c, moved):
        for g in range(groups):
            part = pl.ds(c * pitch + PAD + g * SUB, SUB)
            for n in range(4):
                strips[n][part, :] = jnp.where(halo_lanes, moved[g][n], strips[n][part, :])

    moved = {}
    for c in range(chunks + 2):
        if c < chunks:
            moved[c] = incoming(c)
        if c >= 2:
            insert(c - 2, moved.pop(c - 2))

    def row_at(row, g):
        return pl.ds(PAD + row + g * SUB * pitch, SUB, stride=pitch)

    edge_index = jnp.where(slot < 4, LANES - 4 + slot, jnp.where(slot < 8, 0, jnp.minimum(slot - 8, 3)))
    halo_rows = (
        (0, -2, south, 0), (0, -1, south, 1), (0, rows, north, 0), (0, rows + 1, north, 1),
        (1, -2, south, 2), (1, -1, south, 3), (1, rows, north, 2), (1, rows + 1, north, 3),
        (3, -1, south, 5), (2, rows, north, 4), (3, rows, north, 5),
    )

    def squeeze(x):
        x = jnp.where(mine, x, 0.0)
        for step in (4, 2, 1):
            x = x + pltpu.roll(x, step, 0)
        return x[:1, :]

    def row_pushes(g):
        part = pl.ds(g * SUB, SUB)
        out = []
        for n, row, ref, m in halo_rows:
            value = ref[m, part, :]
            fields[n][row_at(row, g), :] = value
            out.append(pick(value, edge_index))
        index = jnp.full((SUB, LANES), g, jnp.int32)
        return out, pick(corners[0], index), pick(corners[1], index)

    def row_pops(g, pushed):
        values, east, west = pushed
        for (n, row, _, _), value in zip(halo_rows, values):
            if n == 3 and row == -1:
                value = jnp.where(slot == 4, east, value)
            if n == 2:
                value = jnp.where(slot == 7, west, value)
            strips[n][pl.ds(g * pitch + PAD + row, 1), :] = squeeze(value)

    pushed = {}
    for g in range(chunks + 2):
        if g < chunks:
            pushed[g] = row_pushes(g)
        if g >= 2:
            row_pops(g - 2, pushed.pop(g - 2))

    edges = [(0, row, g) for g in range(chunks) for row in (0, 1, rows - 2, rows - 1)]
    edges += [(1, c, g) for c in range(chunks) for g in range(groups)]

    def load(kind, a, g):
        if kind == 0:
            return lambda n, d: fields[n][row_at(a + d, g), :]
        return lambda n, d: strips[n][pl.ds(a * pitch + PAD + g * SUB + d, SUB), :]

    def finish(kind, a, g, held):
        tr_u, tr_v = trends(held)
        if kind == 0:
            part = pl.ds(a + g * SUB * rows, SUB, stride=rows)
            u[part, :] = held[0][2] + ru[part, :] * tr_u
            v[part, :] = held[1][2] + rv[part, :] * tr_v
        else:
            trend_u[a * groups + g] = tr_u
            trend_v[a * groups + g] = tr_v

    pipelined(edges, load, finish)

    keep = slot < 4
    for ref in (trend_u, trend_v):
        for n in range(0, chunks * groups, groups):
            values = [ref[n + g] for g in range(groups)]
            near = [right(x, -4) for x in values]
            for g in range(groups):
                ref[n + g] = jnp.where(keep, values[g], near[g])

    def out_copy(c, n):
        part = pl.ds(c * SUB * rows, SUB * rows)
        return pltpu.make_async_copy((u, v)[n].at[part], (u_hbm, v_hbm)[n].at[part], sems.at[c, n])

    batch = 3 if chunks % 3 == 0 else 1
    at_edge = (lane < 2) | (lane >= LANES - 2)

    def scatter(b, carry):
        units = [(i, s, g) for i in range(batch) for s in range(SUB) for g in range(groups)]
        depth = 4 * DEPTH
        held = []
        for n in range(len(units) + depth):
            if n < len(units):
                i, s, g = units[n]
                c = b * batch + i
                back = LANES - 2 - (SLOT * s + 2)
                held.append((right(trend_u[c * groups + g], back), right(trend_v[c * groups + g], back)))
            if n >= depth:
                i, s, g = units[n - depth]
                c = b * batch + i
                k = c * SUB + s
                own = pl.ds(k * pitch + PAD + g * SUB, SUB)
                part = pl.ds(k * rows + g * SUB, SUB)
                tr_u, tr_v = held[n - depth]
                u[part, :] = jnp.where(at_edge, um[own, :] + ru[part, :] * tr_u, u[part, :])
                v[part, :] = jnp.where(at_edge, vm[own, :] + rv[part, :] * tr_v, v[part, :])
                if s == SUB - 1 and g == groups - 1:
                    out_copy(c, 0).start()
                    out_copy(c, 1).start()
        return carry

    lax.fori_loop(0, chunks // batch, scatter, 0)
    for c in range(chunks):
        out_copy(c, 0).wait()
        out_copy(c, 1).wait()


def exchange(value, pairs):
    return lax.ppermute(value, ("lat", "lon"), pairs)


def local(u, v, eu, ev, su, sv, fu, fv, seam):
    levels, rows, cols = u.shape
    lats, lons = lax.axis_size("lat"), lax.axis_size("lon")
    assert cols == LANES and levels % SUB == 0 and rows % SUB == 0 and lats % 2 == 0 and lons > 1
    pitch = rows + PAD
    groups, chunks = rows // SUB, levels // SUB
    f32 = jnp.float32
    hbm = pl.BlockSpec(memory_space=pltpu.HBM)
    vmem = pl.BlockSpec(memory_space=pltpu.VMEM)
    tile = (SUB, LANES)
    padded = (levels * pitch + PAD, LANES)
    strip = (chunks * pitch + PAD, LANES)
    block = (levels, rows, LANES)
    flat = (levels * rows, LANES)
    line = (6, levels, LANES)
    columns = (chunks * groups,) + tile
    shapes = [padded] * 4 + [flat] * 2 + [strip] * 4 + [line] * 2 + [columns] + [tile] * 2
    outs = [pltpu.VMEM(s, f32) for s in shapes] + [pltpu.VMEM(tile, jnp.int32)]
    packed = pl.pallas_call(
        functools.partial(pack_kernel, levels, rows, lons),
        out_shape=outs,
        in_specs=[hbm] * 9,
        out_specs=[vmem] * len(outs),
        scratch_shapes=[pltpu.VMEM(block, f32)] * 4
        + [pltpu.VMEM(block, jnp.int32)] * 2
        + [pltpu.VMEM((rows, LANES), f32)] * 2
        + [
            pltpu.SMEM(seam.shape, jnp.int32),
            pltpu.SemaphoreType.DMA((chunks, 6)),
            pltpu.SemaphoreType.DMA((3,)),
        ],
        compiler_params=pltpu.CompilerParams(vmem_limit_bytes=16 << 20),
        name="pack",
    )(*(pltpu.with_memory_space_constraint(x, pltpu.HBM) for x in (u, v, eu, ev, su, sv, fu, fv, seam)))
    padded_fields = packed[:4]
    ru, rv = packed[4:6]
    strips = packed[6:10]
    msg_a, msg_b, msg_x, msg_c, msg_d, source = packed[10:]

    def at(k, l):
        return k * lons + l % lons

    every = [(k, l) for k in range(lats) for l in range(lons)]
    to_east = [(at(k, l), at(k, l + 1)) for k, l in every]
    to_west = [(at(k, l), at(k, l - 1)) for k, l in every]
    pair_a = [(at(k, l), at(k ^ 1, l)) for k, l in every]
    pair_c = [(at(k, l), at(k ^ 1, l + 1 if k % 2 else l - 1)) for k, l in every]
    pair_b = []
    pair_d = []
    for k, l in every:
        if k in (0, lats - 1):
            pair_b.append((at(k, l), at(k, l + 1)))
            pair_d.append((at(k, l), at(k, l + 1)))
        elif k % 2:
            pair_b.append((at(k, l), at(k + 1, l)))
            pair_d.append((at(k, l), at(k + 1, l - 1)))
        else:
            pair_b.append((at(k, l), at(k - 1, l)))
            pair_d.append((at(k, l), at(k - 1, l + 1)))
    got_b = exchange(msg_b, pair_b)
    west_x = exchange(msg_x, to_east)
    east_x = west_x if lons == 2 else exchange(msg_x, to_west)
    got_d = exchange(msg_d, pair_d)
    got_c = exchange(msg_c, pair_c)
    got_a = exchange(msg_a, pair_a)
    if lons == 2:
        bands = msg_b
    else:
        bands = lax.all_gather(msg_b, "lon", axis=0, tiled=True)

    points = levels * rows * LANES
    inner = pl.pallas_call(
        functools.partial(inner_kernel, levels, rows),
        out_shape=[pltpu.VMEM(flat, f32)] * 2,
        in_specs=[vmem] * 6,
        out_specs=[vmem] * 2,
        cost_estimate=pl.CostEstimate(flops=60 * points, transcendentals=0, bytes_accessed=32 * points),
        compiler_params=pltpu.CompilerParams(vmem_limit_bytes=16 << 20),
        name="inner",
    )(*padded_fields, ru, rv)

    result = jax.ShapeDtypeStruct(flat, f32)
    done = pl.pallas_call(
        functools.partial(edge_kernel, levels, rows, lons, lats),
        out_shape=[pltpu.VMEM(padded, f32)] * 4 + [pltpu.VMEM(strip, f32)] * 4 + [pltpu.VMEM(flat, f32)] * 2 + [result] * 2,
        in_specs=[vmem] * 20,
        out_specs=[vmem] * 10 + [hbm] * 2,
        input_output_aliases={n: n for n in range(10)},
        scratch_shapes=[
            pltpu.VMEM(line, f32),
            pltpu.VMEM(line, f32),
            pltpu.VMEM((2,) + tile, f32),
            pltpu.VMEM(columns, f32),
            pltpu.VMEM(columns, f32),
            pltpu.SemaphoreType.DMA((chunks, 2)),
        ],
        compiler_params=pltpu.CompilerParams(vmem_limit_bytes=16 << 20),
        name="edge",
    )(*padded_fields, *strips, *inner, ru, rv, got_a, got_b, bands, west_x, east_x, got_c, got_d, source)
    return done[10].reshape(block), done[11].reshape(block)


def solution(mesh):
    tile = P(None, "lat", "lon")
    return jax.shard_map(
        local,
        mesh=mesh,
        in_specs=(tile,) * 4 + (P("lat", "lon"),) * 2 + (tile,) * 2 + (P(),),
        out_specs=(tile, tile),
        check_vma=False,
    )
```

```python
import functools

import jax
import jax.numpy as jnp
from jax import lax
from jax.experimental import pallas as pl
from jax.experimental.pallas import tpu as pltpu
from jax.sharding import PartitionSpec as P


time_step = 0.2
factor = -time_step / 24.0

LANES = 128
SUB = 8
SLOT = 16
DEPTH = 10
PAD = 8


def lane_ids():
    return lax.broadcasted_iota(jnp.int32, (SUB, LANES), 1)


def row_ids():
    return lax.broadcasted_iota(jnp.int32, (SUB, LANES), 0)


def right(x, shift):
    return pltpu.roll(x, shift % LANES, 1)


def strip_slots():
    return lax.rem(lane_ids(), SLOT)


def pack_kernel(
    levels, rows, lons,
    u_hbm, v_hbm, eu_hbm, ev_hbm, su_hbm, sv_hbm, fu_hbm, fv_hbm, seam_hbm,
    um, vm, tu, tv, ru, rv, strip_um, strip_vm, strip_tu, strip_tv,
    msg_b, msg_x, msg_d, msg_c, msg_a, source,
    u, v, eu, ev, fu, fv, su, sv, seam, sems, small_sems,
):
    pitch = rows + PAD
    groups = rows // SUB
    chunks = levels // SUB
    pairs = ((u_hbm, u), (v_hbm, v), (eu_hbm, eu), (ev_hbm, ev), (fu_hbm, fu), (fv_hbm, fv))
    strips = (strip_um, strip_vm, strip_tu, strip_tv)

    def big_copy(c, n):
        part = pl.ds(c * SUB, SUB)
        return pltpu.make_async_copy(pairs[n][0].at[part], pairs[n][1].at[part], sems.at[c, n])

    small = (
        pltpu.make_async_copy(su_hbm, su, small_sems.at[0]),
        pltpu.make_async_copy(sv_hbm, sv, small_sems.at[1]),
        pltpu.make_async_copy(seam_hbm, seam, small_sems.at[2]),
    )
    small[0].start()
    small[1].start()
    ahead = min(4, chunks)
    for c in range(ahead):
        for n in range(6):
            big_copy(c, n).start()
    small[2].start()
    small[0].wait()
    small[1].wait()

    lane = lane_ids()
    slot = strip_slots()

    def chunk(c, carry):
        for n in range(6):
            big_copy(c, n).wait()

        @pl.when(c + ahead < chunks)
        def _():
            for n in range(6):
                big_copy(c + ahead, n).start()

        spans = [(su[pl.ds(g * SUB, SUB), :], sv[pl.ds(g * SUB, SUB), :]) for g in range(groups)]

        def first(g, s):
            k = c * SUB + s
            part = pl.ds(g * SUB, SUB)
            own = pl.ds(k * pitch + PAD + g * SUB, SUB)
            flat = pl.ds(k * rows + g * SUB, SUB)
            flag_u = fu[k, part, :].astype(jnp.float32)
            flag_v = fv[k, part, :].astype(jnp.float32)
            mu = flag_u * u[k, part, :]
            mv = flag_v * v[k, part, :]
            vol_u = spans[g][0] * eu[k, part, :]
            vol_v = spans[g][1] * ev[k, part, :]
            fields = (mu, mv, vol_u * mu, vol_v * mv)
            moved = [right(field, SLOT * s + 4) for field in fields]
            for ref, field in zip((um, vm, tu, tv), fields):
                ref[own, :] = field
            ru[flat, :] = flag_u * (factor / vol_u)
            rv[flat, :] = flag_v * (factor / vol_v)
            return moved

        sums = [None] * 4
        tails = []

        def second(g, s, moved):
            for n in range(4):
                sums[n] = moved[n] if s == 0 else jnp.where(lane >= SLOT * s, moved[n], sums[n])
            if s == SUB - 1:
                tails.append(tuple(sums))

        units = [(g, s) for g in range(groups) for s in range(SUB)]
        held = []
        for i in range(len(units) + DEPTH):
            if i < len(units):
                held.append(first(*units[i]))
            if i >= DEPTH:
                second(*units[i - DEPTH], held[i - DEPTH])
        moved = [
            [
                {by: right(x, by) for by in shifts_by}
                for x, shifts_by in zip(tail, ((-4, 4), (4,), (4, 8), (4, 8)))
            ]
            for tail in tails
        ]
        for g in range(groups):
            for n in range(4):
                part = pl.ds(c * pitch + PAD + g * SUB, SUB)
                strips[n][part, :] = jnp.where(slot < 4, tails[g][n], moved[g][n][4])
            pieces = (
                (2, tails[g][0]), (4, tails[g][1]), (6, moved[g][1][4]),
                (8, moved[g][2][4]), (10, moved[g][2][8]), (12, moved[g][3][8]),
            )
            packed = moved[g][0][-4]
            for first_slot, piece in pieces:
                packed = jnp.where(slot >= first_slot, piece, packed)
            msg_x[c * groups + g] = packed
        return carry

    lax.fori_loop(0, chunks, chunk, 0)

    def row_of(ref, row):
        return ref[pl.ds(PAD + row, levels, stride=pitch), :]

    def pack_rows(ref, top):
        if top:
            picks = ((um, rows - 2), (um, rows - 1), (vm, rows - 2), (vm, rows - 1), (tu, rows - 1), (tv, rows - 1))
        else:
            picks = ((um, 0), (um, 1), (vm, 0), (vm, 1), (tu, 0), (tv, 0))
        for n, (field, row) in enumerate(picks):
            ref[n] = row_of(field, row)

    def pack_corner(ref, top):
        line = row_of(tv, rows - 1) if top else row_of(tu, 0)
        moved = [right(line[g * SUB : (g + 1) * SUB, :], g if top else g + 1) for g in range(chunks)]
        packed = moved[0]
        for g in range(1, chunks):
            packed = jnp.where(lane == g, moved[g], packed)
        ref[...] = packed

    odd = lax.rem(lax.axis_index("lat"), 2)

    @pl.when(odd == 0)
    def _():
        pack_corner(msg_c, True)
        pack_corner(msg_d, False)
        pack_rows(msg_a, True)
        pack_rows(msg_b, False)

    @pl.when(odd == 1)
    def _():
        pack_corner(msg_c, False)
        pack_corner(msg_d, True)
        pack_rows(msg_a, False)
        pack_rows(msg_b, True)

    small[2].wait()
    ring = lons * LANES
    where = seam[0] - lax.axis_index("lon") * LANES - lane
    source[...] = jnp.where(where < 0, where + ring, where)


def start_unit(load, with_below):
    h = {"load": load}
    h["mu_east"] = right(load(0, 0), -1)
    h["mv_west"] = right(load(1, 0), 1)
    h["t_west"] = right(load(2, 0), 1)
    h["c_east"] = right(load(3, 0), -1)
    if with_below:
        h["below_east"] = right(load(3, -1), -1)
    return h


def middle_unit(h):
    mu, mv = h["load"](0, 0), h["load"](1, 0)
    h["far_u"] = right(7.0 * h["mu_east"] - mu, 2)
    h["near_u"] = 7.0 * mu - h.pop("mu_east")
    h["far_v"] = right(7.0 * h["mv_west"] - mv, -2)
    h["near_v"] = 7.0 * mv - h.pop("mv_west")


def last_unit(h):
    t0 = h["load"](2, 0)
    flux_u = (h.pop("t_west") + t0) * (h.pop("near_u") + h.pop("far_u"))
    flux_v = (t0 + h["load"](2, 1)) * (h.pop("near_v") + h.pop("far_v"))
    h["flux_u"] = flux_u
    h["flux_v"] = flux_v
    h["flux_u_east"] = right(flux_u, -1)
    h["flux_v_west"] = right(flux_v, 1)


def across(pair, a, b, c, d):
    return pair * (7.0 * (b + c) - (a + d))


def row_terms(h, with_below):
    load = h["load"]
    mu = [load(0, d) for d in range(-2, 3)]
    mv = [load(1, d) for d in range(-2, 3)]
    below, c0 = load(3, -1), load(3, 0)
    dy = across(c0 + h["c_east"], *mu[1:])
    if with_below:
        dy = dy - across(below + h["below_east"], *mu[:4])
    ey = across(c0 + load(3, 1), *mv[1:]) - across(below + c0, *mv[:4])
    return mu[2], mv[2], dy, h["flux_v"] - h["flux_v_west"] + ey, h["flux_u_east"] - h["flux_u"]


def pipelined(units, load, finish, with_below=True):
    held = []
    for i in range(len(units) + 3 * DEPTH):
        if i < len(units):
            held.append(start_unit(load(*units[i]), with_below))
        if 0 <= i - DEPTH < len(units):
            middle_unit(held[i - DEPTH])
        if 0 <= i - 2 * DEPTH < len(units):
            last_unit(held[i - 2 * DEPTH])
        if i >= 3 * DEPTH:
            finish(*units[i - 3 * DEPTH], held[i - 3 * DEPTH])
            held[i - 3 * DEPTH] = None


def inner_kernel(levels, rows, um, vm, tu, tv, ru, rv, u, v):
    pitch = rows + PAD
    groups = rows // SUB
    fields = (um, vm, tu, tv)
    sub = row_ids()

    def chunk(c, carry):
        def load(s, g):
            base = (c * SUB + s) * pitch + PAD + g * SUB
            return lambda n, d: fields[n][pl.ds(base + d, SUB), :]

        last = [None]

        def finish(s, g, h):
            part = pl.ds((c * SUB + s) * rows + g * SUB, SUB)
            mu, mv, north_flux, trend_v, dx = row_terms(h, False)
            moved = pltpu.roll(north_flux, 1, 0)
            dy = north_flux - (jnp.where(sub == 0, last[0], moved) if g else moved)
            last[0] = moved
            u[part, :] = mu + ru[part, :] * (dx + dy)
            v[part, :] = mv + rv[part, :] * trend_v

        pipelined([(s, g) for s in range(SUB) for g in range(groups)], load, finish, False)
        return carry

    lax.fori_loop(0, levels // SUB, chunk, 0)


def edge_kernel(
    levels, rows, lons, tops,
    um_in, vm_in, tu_in, tv_in, strip_um_in, strip_vm_in, strip_tu_in, strip_tv_in, u_in, v_in,
    ru, rv, got_b, west_x, east_x, got_d, got_c, got_a, bands, source,
    um, vm, tu, tv, strip_um, strip_vm, strip_tu, strip_tv, u, v, u_hbm, v_hbm,
    south, north, corners, trend_u, trend_v, sems,
):
    pitch = rows + PAD
    groups = rows // SUB
    chunks = levels // SUB
    lane = lane_ids()
    sub = row_ids()
    slot = strip_slots()
    mine = lax.div(lane, SLOT) == sub
    at = lax.axis_index("lat")
    odd = lax.rem(at, 2)
    is_top = at == tops - 1
    fields = (um, vm, tu, tv)
    strips = (strip_um, strip_vm, strip_tu, strip_tv)

    def pick(x, index):
        return jnp.take_along_axis(x, index, axis=1, mode="promise_in_bounds")

    @pl.when(odd == 0)
    def _():
        keep = at > 0
        for n in range(6):
            south[n] = jnp.where(keep, got_b[n], 0.0)
            north[n] = got_a[n]
        corners[0] = jnp.where(keep, got_d[...], 0.0)
        corners[1] = got_c[...]

    @pl.when(odd == 1)
    def _():
        for n in range(6):
            south[n] = got_a[n]
        corners[0] = got_c[...]

    @pl.when(jnp.logical_and(odd == 1, jnp.logical_not(is_top)))
    def _():
        for n in range(6):
            north[n] = got_b[n]
        corners[1] = got_d[...]

    @pl.when(is_top)
    def _():
        here = source[...]
        ring = lons * LANES
        before = jnp.where(here + 1 >= ring, 0, here + 1)
        column = lax.axis_index("lon")

        def mirrored(row, part, spot):
            within = lax.rem(spot, LANES)
            tile = lax.div(spot, LANES)
            out = jnp.zeros((SUB, LANES), jnp.float32)
            if lons == 2:
                sheets = ((column, bands[row, part, :]), (1 - column, got_b[row, part, :]))
            else:
                sheets = tuple((t, bands[t * 6 + row, part, :]) for t in range(lons))
            for t, sheet in sheets:
                out = jnp.where(tile == t, pick(sheet, within), out)
            return -out

        packed = jnp.zeros((SUB, LANES), jnp.float32)
        for g in range(chunks):
            part = pl.ds(g * SUB, SUB)
            for n, row in enumerate((1, 0, 3, 2, 4, 5)):
                north[n, part, :] = mirrored(row, part, here)
            packed = jnp.where(lane == g, right(mirrored(4, part, before), g), packed)
        corners[1] = packed

    from_west = lax.rem(lane, 4) >= 2
    halo_lanes = (slot >= 4) & (slot < 8)

    def incoming(c):
        out = []
        for g in range(groups):
            got = west_x[c * groups + g]
            if lons > 2:
                got = jnp.where(from_west, got, east_x[c * groups + g])
            out.append([right(got, 4 - 4 * n) for n in range(4)])
        return out

    def insert(c, moved):
        for g in range(groups):
            part = pl.ds(c * pitch + PAD + g * SUB, SUB)
            for n in range(4):
                strips[n][part, :] = jnp.where(halo_lanes, moved[g][n], strips[n][part, :])

    moved = {}
    for c in range(chunks + 2):
        if c < chunks:
            moved[c] = incoming(c)
        if c >= 2:
            insert(c - 2, moved.pop(c - 2))

    def row_at(row, g):
        return pl.ds(PAD + row + g * SUB * pitch, SUB, stride=pitch)

    edge_index = jnp.where(slot < 4, LANES - 4 + slot, jnp.where(slot < 8, 0, jnp.minimum(slot - 8, 3)))
    halo_rows = (
        (0, -2, south, 0), (0, -1, south, 1), (0, rows, north, 0), (0, rows + 1, north, 1),
        (1, -2, south, 2), (1, -1, south, 3), (1, rows, north, 2), (1, rows + 1, north, 3),
        (3, -1, south, 5), (2, rows, north, 4), (3, rows, north, 5),
    )

    def squeeze(x):
        x = jnp.where(mine, x, 0.0)
        for step in (4, 2, 1):
            x = x + pltpu.roll(x, step, 0)
        return x[:1, :]

    def row_pushes(g):
        part = pl.ds(g * SUB, SUB)
        out = []
        for n, row, ref, m in halo_rows:
            value = ref[m, part, :]
            fields[n][row_at(row, g), :] = value
            out.append(pick(value, edge_index))
        index = jnp.full((SUB, LANES), g, jnp.int32)
        return out, pick(corners[0], index), pick(corners[1], index)

    def row_pops(g, pushed):
        values, east, west = pushed
        for (n, row, _, _), value in zip(halo_rows, values):
            if n == 3 and row == -1:
                value = jnp.where(slot == 4, east, value)
            if n == 2:
                value = jnp.where(slot == 7, west, value)
            strips[n][pl.ds(g * pitch + PAD + row, 1), :] = squeeze(value)

    pushed = {}
    for g in range(chunks + 2):
        if g < chunks:
            pushed[g] = row_pushes(g)
        if g >= 2:
            row_pops(g - 2, pushed.pop(g - 2))

    edges = [(0, row, g) for g in range(chunks) for row in (0, 1, rows - 2, rows - 1)]
    edges += [(1, c, g) for c in range(chunks) for g in range(groups)]

    def load(kind, a, g):
        if kind == 0:
            return lambda n, d: fields[n][row_at(a + d, g), :]
        return lambda n, d: strips[n][pl.ds(a * pitch + PAD + g * SUB + d, SUB), :]

    def finish(kind, a, g, held):
        mu, mv, dy, tr_v, dx = row_terms(held, True)
        tr_u = dx + dy
        if kind == 0:
            part = pl.ds(a + g * SUB * rows, SUB, stride=rows)
            u[part, :] = mu + ru[part, :] * tr_u
            v[part, :] = mv + rv[part, :] * tr_v
        else:
            trend_u[a * groups + g] = tr_u
            trend_v[a * groups + g] = tr_v

    pipelined(edges, load, finish)

    keep = slot < 4
    for ref in (trend_u, trend_v):
        for n in range(0, chunks * groups, groups):
            values = [ref[n + g] for g in range(groups)]
            near = [right(x, -4) for x in values]
            for g in range(groups):
                ref[n + g] = jnp.where(keep, values[g], near[g])

    def out_copy(c, n):
        part = pl.ds(c * SUB * rows, SUB * rows)
        return pltpu.make_async_copy((u, v)[n].at[part], (u_hbm, v_hbm)[n].at[part], sems.at[c, n])

    batch = 3 if chunks % 3 == 0 else 1
    at_edge = (lane < 2) | (lane >= LANES - 2)

    def scatter(b, carry):
        units = [(i, s, g) for i in range(batch) for s in range(SUB) for g in range(groups)]
        depth = 4 * DEPTH
        held = []
        for n in range(len(units) + depth):
            if n < len(units):
                i, s, g = units[n]
                c = b * batch + i
                back = LANES - 2 - (SLOT * s + 2)
                held.append((right(trend_u[c * groups + g], back), right(trend_v[c * groups + g], back)))
            if n >= depth:
                i, s, g = units[n - depth]
                c = b * batch + i
                k = c * SUB + s
                own = pl.ds(k * pitch + PAD + g * SUB, SUB)
                part = pl.ds(k * rows + g * SUB, SUB)
                tr_u, tr_v = held[n - depth]
                u[part, :] = jnp.where(at_edge, um[own, :] + ru[part, :] * tr_u, u[part, :])
                v[part, :] = jnp.where(at_edge, vm[own, :] + rv[part, :] * tr_v, v[part, :])
                if s == SUB - 1 and g == groups - 1:
                    out_copy(c, 0).start()
                    out_copy(c, 1).start()
        return carry

    lax.fori_loop(0, chunks // batch, scatter, 0)
    for c in range(chunks):
        out_copy(c, 0).wait()
        out_copy(c, 1).wait()


def exchange(value, pairs):
    return lax.ppermute(value, ("lat", "lon"), pairs)


def local(u, v, eu, ev, su, sv, fu, fv, seam):
    levels, rows, cols = u.shape
    lats, lons = lax.axis_size("lat"), lax.axis_size("lon")
    assert cols == LANES and levels % SUB == 0 and rows % SUB == 0 and lats % 2 == 0 and lons > 1
    pitch = rows + PAD
    groups, chunks = rows // SUB, levels // SUB
    f32 = jnp.float32
    hbm = pl.BlockSpec(memory_space=pltpu.HBM)
    vmem = pl.BlockSpec(memory_space=pltpu.VMEM)
    tile = (SUB, LANES)
    padded = (levels * pitch + PAD, LANES)
    strip = (chunks * pitch + PAD, LANES)
    block = (levels, rows, LANES)
    flat = (levels * rows, LANES)
    line = (6, levels, LANES)
    columns = (chunks * groups,) + tile
    shapes = [padded] * 4 + [flat] * 2 + [strip] * 4 + [line, columns, tile, tile, line]
    outs = [pltpu.VMEM(s, f32) for s in shapes] + [pltpu.VMEM(tile, jnp.int32)]
    packed = pl.pallas_call(
        functools.partial(pack_kernel, levels, rows, lons),
        out_shape=outs,
        in_specs=[hbm] * 9,
        out_specs=[vmem] * len(outs),
        scratch_shapes=[pltpu.VMEM(block, f32)] * 4
        + [pltpu.VMEM(block, jnp.int32)] * 2
        + [pltpu.VMEM((rows, LANES), f32)] * 2
        + [
            pltpu.SMEM(seam.shape, jnp.int32),
            pltpu.SemaphoreType.DMA((chunks, 6)),
            pltpu.SemaphoreType.DMA((3,)),
        ],
        compiler_params=pltpu.CompilerParams(vmem_limit_bytes=16 << 20),
        name="pack",
    )(*(pltpu.with_memory_space_constraint(x, pltpu.HBM) for x in (u, v, eu, ev, su, sv, fu, fv, seam)))
    padded_fields = packed[:4]
    ru, rv = packed[4:6]
    strips = packed[6:10]
    msg_b, msg_x, msg_d, msg_c, msg_a, source = packed[10:]

    def at(k, l):
        return k * lons + l % lons

    every = [(k, l) for k in range(lats) for l in range(lons)]
    to_east = [(at(k, l), at(k, l + 1)) for k, l in every]
    to_west = [(at(k, l), at(k, l - 1)) for k, l in every]
    pair_a = [(at(k, l), at(k ^ 1, l)) for k, l in every]
    pair_c = [(at(k, l), at(k ^ 1, l + 1 if k % 2 else l - 1)) for k, l in every]
    pair_b = []
    pair_d = []
    for k, l in every:
        if k in (0, lats - 1):
            pair_b.append((at(k, l), at(k, l + 1)))
            pair_d.append((at(k, l), at(k, l + 1)))
        elif k % 2:
            pair_b.append((at(k, l), at(k + 1, l)))
            pair_d.append((at(k, l), at(k + 1, l - 1)))
        else:
            pair_b.append((at(k, l), at(k - 1, l)))
            pair_d.append((at(k, l), at(k - 1, l + 1)))
    got_b = exchange(msg_b, pair_b)
    west_x = exchange(msg_x, to_east)
    east_x = west_x if lons == 2 else exchange(msg_x, to_west)
    got_d = exchange(msg_d, pair_d)
    got_c = exchange(msg_c, pair_c)
    got_a = exchange(msg_a, pair_a)
    if lons == 2:
        bands = msg_b
    else:
        bands = lax.all_gather(msg_b, "lon", axis=0, tiled=True)

    points = levels * rows * LANES
    inner = pl.pallas_call(
        functools.partial(inner_kernel, levels, rows),
        out_shape=[pltpu.VMEM(flat, f32)] * 2,
        in_specs=[vmem] * 6,
        out_specs=[vmem] * 2,
        cost_estimate=pl.CostEstimate(flops=60 * points, transcendentals=0, bytes_accessed=32 * points),
        compiler_params=pltpu.CompilerParams(vmem_limit_bytes=16 << 20),
        name="inner",
    )(*padded_fields, ru, rv)

    result = jax.ShapeDtypeStruct(flat, f32)
    done = pl.pallas_call(
        functools.partial(edge_kernel, levels, rows, lons, lats),
        out_shape=[pltpu.VMEM(padded, f32)] * 4 + [pltpu.VMEM(strip, f32)] * 4 + [pltpu.VMEM(flat, f32)] * 2 + [result] * 2,
        in_specs=[vmem] * 20,
        out_specs=[vmem] * 10 + [hbm] * 2,
        input_output_aliases={n: n for n in range(10)},
        scratch_shapes=[
            pltpu.VMEM(line, f32),
            pltpu.VMEM(line, f32),
            pltpu.VMEM((2,) + tile, f32),
            pltpu.VMEM(columns, f32),
            pltpu.VMEM(columns, f32),
            pltpu.SemaphoreType.DMA((chunks, 2)),
        ],
        compiler_params=pltpu.CompilerParams(vmem_limit_bytes=16 << 20),
        name="edge",
    )(*padded_fields, *strips, *inner, ru, rv, got_b, west_x, east_x, got_d, got_c, got_a, bands, source)
    return done[10].reshape(block), done[11].reshape(block)


def solution(mesh):
    tile = P(None, "lat", "lon")
    return jax.shard_map(
        local,
        mesh=mesh,
        in_specs=(tile,) * 4 + (P("lat", "lon"),) * 2 + (tile,) * 2 + (P(),),
        out_specs=(tile, tile),
        check_vma=False,
    )
```

```python
import functools

import jax
import jax.numpy as jnp
from jax import lax
from jax.experimental import pallas as pl
from jax.experimental.pallas import tpu as pltpu
from jax.sharding import PartitionSpec as P


time_step = 0.2
factor = -time_step / 24.0

LANES = 128
SUB = 8
SLOT = 16
DEPTH = 10
PAD = 8


def lane_ids():
    return lax.broadcasted_iota(jnp.int32, (SUB, LANES), 1)


def row_ids():
    return lax.broadcasted_iota(jnp.int32, (SUB, LANES), 0)


def right(x, shift):
    return pltpu.roll(x, shift % LANES, 1)


def strip_slots():
    return lax.rem(lane_ids(), SLOT)


def pack_kernel(
    levels, rows, lons,
    u_hbm, v_hbm, eu_hbm, ev_hbm, su_hbm, sv_hbm, fu_hbm, fv_hbm, seam_hbm,
    um, vm, tu, tv, ru, rv, strip_um, strip_vm, strip_tu, strip_tv,
    msg_b, msg_x, msg_d, msg_c, msg_a, source,
    u, v, eu, ev, fu, fv, su, sv, seam, sems, small_sems,
):
    pitch = rows + PAD
    groups = rows // SUB
    chunks = levels // SUB
    pairs = ((u_hbm, u), (v_hbm, v), (eu_hbm, eu), (ev_hbm, ev), (fu_hbm, fu), (fv_hbm, fv))
    strips = (strip_um, strip_vm, strip_tu, strip_tv)

    def big_copy(c, n):
        part = pl.ds(c * SUB, SUB)
        return pltpu.make_async_copy(pairs[n][0].at[part], pairs[n][1].at[part], sems.at[c, n])

    small = (
        pltpu.make_async_copy(su_hbm, su, small_sems.at[0]),
        pltpu.make_async_copy(sv_hbm, sv, small_sems.at[1]),
        pltpu.make_async_copy(seam_hbm, seam, small_sems.at[2]),
    )
    small[0].start()
    small[1].start()
    ahead = min(6, chunks)
    for c in range(ahead):
        for n in range(6):
            big_copy(c, n).start()
    small[2].start()
    small[0].wait()
    small[1].wait()

    lane = lane_ids()
    slot = strip_slots()

    def arrive(c):
        for n in range(6):
            big_copy(c, n).wait()

    def request(c):
        for n in range(6):
            big_copy(c, n).start()

    spans = [(su[pl.ds(g * SUB, SUB), :], sv[pl.ds(g * SUB, SUB), :]) for g in range(groups)]
    units = [(g, s) for g in range(groups) for s in range(SUB)]
    padded = (um, vm, tu, tv)

    def mask(base, c):
        for g, s in units:
            k = c * SUB + s
            part = pl.ds(g * SUB, SUB)
            own = pl.ds(base + s * pitch + PAD + g * SUB, SUB)
            flat = pl.ds(k * rows + g * SUB, SUB)
            flag_u = fu[k, part, :].astype(jnp.float32)
            flag_v = fv[k, part, :].astype(jnp.float32)
            mu = flag_u * u[k, part, :]
            mv = flag_v * v[k, part, :]
            vol_u = spans[g][0] * eu[k, part, :]
            vol_v = spans[g][1] * ev[k, part, :]
            um[own, :] = mu
            vm[own, :] = mv
            tu[own, :] = vol_u * mu
            tv[own, :] = vol_v * mv
            ru[flat, :] = flag_u * (factor / vol_u)
            rv[flat, :] = flag_v * (factor / vol_v)

    def edge_shifts(base):
        return [
            [right(field[pl.ds(base + s * pitch + PAD + g * SUB, SUB), :], SLOT * s + 4) for field in padded]
            for g, s in units
        ]

    def edge_merge(base, moved):
        for g in range(groups):
            for n in range(4):
                total = moved[g * SUB][n]
                for s in range(1, SUB):
                    total = jnp.where(lane >= SLOT * s, moved[g * SUB + s][n], total)
                strips[n][pl.ds(base + PAD + g * SUB, SUB), :] = total

    arrive(0)
    if ahead < chunks:
        request(ahead)
    mask(0, 0)

    def chunk(c, carry):
        arrive(c)

        @pl.when(c + ahead < chunks)
        def _():
            request(c + ahead)

        base = pl.multiple_of(c * (SUB * pitch), SUB)
        moved = edge_shifts(base - SUB * pitch)
        mask(base, c)
        edge_merge(pl.multiple_of(c * pitch, SUB) - pitch, moved)
        return carry

    lax.fori_loop(1, chunks, chunk, 0)
    edge_merge((chunks - 1) * pitch, edge_shifts((chunks - 1) * SUB * pitch))

    shifts_by = ((-4, 4), (4,), (4, 8), (4, 5))

    def raw(c, g, n):
        return strips[n][pl.ds(c * pitch + PAD + g * SUB, SUB), :]

    sets = [(c, j) for c in range(chunks) for j in range(groups // 4)]

    def message_shifts(c, j):
        return [[{by: right(raw(c, 4 * j + g, n), by) for by in shifts_by[n]} for n in range(4)] for g in range(4)]

    def message_rows(c, j, moved):
        out = []
        for g in range(4):
            fields = [raw(c, 4 * j + g, n) for n in range(4)]
            packed = moved[g][0][-4]
            for first_slot, piece in (
                (2, fields[0]), (4, fields[1]), (6, moved[g][1][4]),
                (8, moved[g][2][4]), (9, moved[g][3][5]), (10, moved[g][2][8]),
            ):
                packed = jnp.where(slot >= first_slot, piece, packed)
            out.append(packed)
            for n in range(4):
                part = pl.ds(c * pitch + PAD + (4 * j + g) * SUB, SUB)
                strips[n][part, :] = jnp.where(slot < 4, fields[n], moved[g][n][4])
        return out[:3], [right(out[3], 12 - 4 * q) for q in range(3)]

    def message_store(c, j, rows_of, rest):
        for q in range(3):
            msg_x[(c * (groups // 4) + j) * 3 + q] = jnp.where(slot >= 12, rest[q], rows_of[q])

    one, two = {}, {}
    for i in range(len(sets) + 4):
        if i < len(sets):
            one[i] = message_shifts(*sets[i])
        if 0 <= i - 2 < len(sets):
            two[i - 2] = message_rows(*sets[i - 2], one.pop(i - 2))
        if i >= 4:
            message_store(*sets[i - 4], *two.pop(i - 4))

    def row_of(ref, row):
        return ref[pl.ds(PAD + row, levels, stride=pitch), :]

    def pack_rows(ref, top):
        if top:
            picks = ((um, rows - 2), (um, rows - 1), (vm, rows - 2), (vm, rows - 1), (tu, rows - 1), (tv, rows - 1))
        else:
            picks = ((um, 0), (um, 1), (vm, 0), (vm, 1), (tu, 0), (tv, 0))
        for n, (field, row) in enumerate(picks):
            ref[n] = row_of(field, row)

    def pack_corner(ref, top):
        line = row_of(tv, rows - 1) if top else row_of(tu, 0)
        moved = [right(line[g * SUB : (g + 1) * SUB, :], g if top else g + 1) for g in range(chunks)]
        packed = moved[0]
        for g in range(1, chunks):
            packed = jnp.where(lane == g, moved[g], packed)
        ref[...] = packed

    odd = lax.rem(lax.axis_index("lat"), 2)

    @pl.when(odd == 0)
    def _():
        pack_corner(msg_c, True)
        pack_corner(msg_d, False)
        pack_rows(msg_a, True)
        pack_rows(msg_b, False)

    @pl.when(odd == 1)
    def _():
        pack_corner(msg_c, False)
        pack_corner(msg_d, True)
        pack_rows(msg_a, False)
        pack_rows(msg_b, True)

    small[2].wait()
    ring = lons * LANES
    where = seam[0] - lax.axis_index("lon") * LANES - lane
    source[...] = jnp.where(where < 0, where + ring, where)


def start_unit(load, with_below):
    h = {"load": load}
    h["mu_east"] = right(load(0, 0), -1)
    h["mv_west"] = right(load(1, 0), 1)
    h["t_west"] = right(load(2, 0), 1)
    h["c_east"] = right(load(3, 0), -1)
    if with_below:
        h["below_east"] = right(load(3, -1), -1)
    return h


def middle_unit(h):
    mu, mv = h["load"](0, 0), h["load"](1, 0)
    h["far_u"] = right(7.0 * h["mu_east"] - mu, 2)
    h["near_u"] = 7.0 * mu - h.pop("mu_east")
    h["far_v"] = right(7.0 * h["mv_west"] - mv, -2)
    h["near_v"] = 7.0 * mv - h.pop("mv_west")


def last_unit(h):
    t0 = h["load"](2, 0)
    flux_u = (h.pop("t_west") + t0) * (h.pop("near_u") + h.pop("far_u"))
    flux_v = (t0 + h["load"](2, 1)) * (h.pop("near_v") + h.pop("far_v"))
    h["flux_u"] = flux_u
    h["flux_v"] = flux_v
    h["flux_u_east"] = right(flux_u, -1)
    h["flux_v_west"] = right(flux_v, 1)


def across(pair, a, b, c, d):
    return pair * (7.0 * (b + c) - (a + d))


def row_terms(h, with_below):
    load = h["load"]
    mu = [load(0, d) for d in range(-2, 3)]
    mv = [load(1, d) for d in range(-2, 3)]
    below, c0 = load(3, -1), load(3, 0)
    dy = across(c0 + h["c_east"], *mu[1:])
    if with_below:
        dy = dy - across(below + h["below_east"], *mu[:4])
    ey = across(c0 + load(3, 1), *mv[1:]) - across(below + c0, *mv[:4])
    return mu[2], mv[2], dy, h["flux_v"] - h["flux_v_west"] + ey, h["flux_u_east"] - h["flux_u"]


def pipelined(units, load, finish, with_below=True):
    held = []
    for i in range(len(units) + 3 * DEPTH):
        if i < len(units):
            held.append(start_unit(load(*units[i]), with_below))
        if 0 <= i - DEPTH < len(units):
            middle_unit(held[i - DEPTH])
        if 0 <= i - 2 * DEPTH < len(units):
            last_unit(held[i - 2 * DEPTH])
        if i >= 3 * DEPTH:
            finish(*units[i - 3 * DEPTH], held[i - 3 * DEPTH])
            held[i - 3 * DEPTH] = None


def inner_kernel(levels, rows, um, vm, tu, tv, ru, rv, u, v):
    pitch = rows + PAD
    groups = rows // SUB
    fields = (um, vm, tu, tv)
    sub = row_ids()

    def chunk(c, carry):
        def load(s, g):
            base = (c * SUB + s) * pitch + PAD + g * SUB
            return lambda n, d: fields[n][pl.ds(base + d, SUB), :]

        last = [None]

        def finish(s, g, h):
            part = pl.ds((c * SUB + s) * rows + g * SUB, SUB)
            mu, mv, north_flux, trend_v, dx = row_terms(h, False)
            moved = pltpu.roll(north_flux, 1, 0)
            dy = north_flux - (jnp.where(sub == 0, last[0], moved) if g else moved)
            last[0] = moved
            u[part, :] = mu + ru[part, :] * (dx + dy)
            v[part, :] = mv + rv[part, :] * trend_v

        pipelined([(s, g) for s in range(SUB) for g in range(groups)], load, finish, False)
        return carry

    lax.fori_loop(0, levels // SUB, chunk, 0)


def edge_kernel(
    levels, rows, lons, tops,
    um_in, vm_in, tu_in, tv_in, strip_um_in, strip_vm_in, strip_tu_in, strip_tv_in, u_in, v_in,
    ru, rv, got_b, west_x, east_x, got_d, got_c, got_a, bands, source,
    um, vm, tu, tv, strip_um, strip_vm, strip_tu, strip_tv, u, v, u_hbm, v_hbm,
    south, north, corners, trend_u, trend_v, sems,
):
    pitch = rows + PAD
    groups = rows // SUB
    chunks = levels // SUB
    lane = lane_ids()
    sub = row_ids()
    slot = strip_slots()
    mine = lax.div(lane, SLOT) == sub
    at = lax.axis_index("lat")
    odd = lax.rem(at, 2)
    is_top = at == tops - 1
    fields = (um, vm, tu, tv)
    strips = (strip_um, strip_vm, strip_tu, strip_tv)

    def pick(x, index):
        return jnp.take_along_axis(x, index, axis=1, mode="promise_in_bounds")

    @pl.when(odd == 0)
    def _():
        keep = at > 0
        for n in range(6):
            south[n] = jnp.where(keep, got_b[n], 0.0)
            north[n] = got_a[n]
        corners[0] = jnp.where(keep, got_d[...], 0.0)
        corners[1] = got_c[...]

    @pl.when(odd == 1)
    def _():
        for n in range(6):
            south[n] = got_a[n]
        corners[0] = got_c[...]

    @pl.when(jnp.logical_and(odd == 1, jnp.logical_not(is_top)))
    def _():
        for n in range(6):
            north[n] = got_b[n]
        corners[1] = got_d[...]

    @pl.when(is_top)
    def _():
        here = source[...]
        ring = lons * LANES
        before = jnp.where(here + 1 >= ring, 0, here + 1)
        column = lax.axis_index("lon")

        def mirrored(row, part, spot):
            within = lax.rem(spot, LANES)
            tile = lax.div(spot, LANES)
            out = jnp.zeros((SUB, LANES), jnp.float32)
            if lons == 2:
                sheets = ((column, bands[row, part, :]), (1 - column, got_b[row, part, :]))
            else:
                sheets = tuple((t, bands[t * 6 + row, part, :]) for t in range(lons))
            for t, sheet in sheets:
                out = jnp.where(tile == t, pick(sheet, within), out)
            return -out

        packed = jnp.zeros((SUB, LANES), jnp.float32)
        for g in range(chunks):
            part = pl.ds(g * SUB, SUB)
            for n, row in enumerate((1, 0, 3, 2, 4, 5)):
                north[n, part, :] = mirrored(row, part, here)
            packed = jnp.where(lane == g, right(mirrored(4, part, before), g), packed)
        corners[1] = packed

    from_west = lax.rem(lane, 4) >= 2
    halo_lanes = (slot >= 4) & (slot < 8)

    def incoming(c):
        out = []
        for j in range(groups // 4):
            got = []
            for q in range(3):
                piece = west_x[(c * (groups // 4) + j) * 3 + q]
                if lons > 2:
                    piece = jnp.where(from_west, piece, east_x[(c * (groups // 4) + j) * 3 + q])
                got.append(piece)
            for x in got:
                out.append([right(x, 4), x, right(x, -4), right(x, -5)])
            out.append([right(got[0], -8), right(got[1], -8), right(got[2], -8), right(got[2], -9)])
        return out

    def insert(c, moved):
        for g in range(groups):
            part = pl.ds(c * pitch + PAD + g * SUB, SUB)
            for n in range(4):
                strips[n][part, :] = jnp.where(halo_lanes, moved[g][n], strips[n][part, :])

    moved = {}
    for c in range(chunks + 2):
        if c < chunks:
            moved[c] = incoming(c)
        if c >= 2:
            insert(c - 2, moved.pop(c - 2))

    def row_at(row, g):
        return pl.ds(PAD + row + g * SUB * pitch, SUB, stride=pitch)

    edge_index = jnp.where(slot < 4, LANES - 4 + slot, jnp.where(slot < 8, 0, jnp.minimum(slot - 8, 3)))
    halo_rows = (
        (0, -2, south, 0), (0, -1, south, 1), (0, rows, north, 0), (0, rows + 1, north, 1),
        (1, -2, south, 2), (1, -1, south, 3), (1, rows, north, 2), (1, rows + 1, north, 3),
        (3, -1, south, 5), (2, rows, north, 4), (3, rows, north, 5),
    )

    def squeeze(x):
        x = jnp.where(mine, x, 0.0)
        for step in (4, 2, 1):
            x = x + pltpu.roll(x, step, 0)
        return x[:1, :]

    def row_pushes(g):
        part = pl.ds(g * SUB, SUB)
        out = []
        for n, row, ref, m in halo_rows:
            value = ref[m, part, :]
            fields[n][row_at(row, g), :] = value
            out.append(pick(value, edge_index))
        index = jnp.full((SUB, LANES), g, jnp.int32)
        return out, pick(corners[0], index), pick(corners[1], index)

    def row_pops(g, pushed):
        values, east, west = pushed
        for (n, row, _, _), value in zip(halo_rows, values):
            if n == 3 and row == -1:
                value = jnp.where(slot == 4, east, value)
            if n == 2:
                value = jnp.where(slot == 7, west, value)
            strips[n][pl.ds(g * pitch + PAD + row, 1), :] = squeeze(value)

    pushed = {}
    for g in range(chunks + 2):
        if g < chunks:
            pushed[g] = row_pushes(g)
        if g >= 2:
            row_pops(g - 2, pushed.pop(g - 2))

    edges = [(0, row, g) for g in range(chunks) for row in (0, 1, rows - 2, rows - 1)]
    edges += [(1, c, g) for c in range(chunks) for g in range(groups)]

    def load(kind, a, g):
        if kind == 0:
            return lambda n, d: fields[n][row_at(a + d, g), :]
        return lambda n, d: strips[n][pl.ds(a * pitch + PAD + g * SUB + d, SUB), :]

    def finish(kind, a, g, held):
        mu, mv, dy, tr_v, dx = row_terms(held, True)
        tr_u = dx + dy
        if kind == 0:
            part = pl.ds(a + g * SUB * rows, SUB, stride=rows)
            u[part, :] = mu + ru[part, :] * tr_u
            v[part, :] = mv + rv[part, :] * tr_v
        else:
            trend_u[a * groups + g] = tr_u
            trend_v[a * groups + g] = tr_v

    pipelined(edges, load, finish)

    keep = slot < 4
    for ref in (trend_u, trend_v):
        for n in range(0, chunks * groups, groups):
            values = [ref[n + g] for g in range(groups)]
            near = [right(x, -4) for x in values]
            for g in range(groups):
                ref[n + g] = jnp.where(keep, values[g], near[g])

    def out_copy(c, n):
        part = pl.ds(c * SUB * rows, SUB * rows)
        return pltpu.make_async_copy((u, v)[n].at[part], (u_hbm, v_hbm)[n].at[part], sems.at[c, n])

    batch = chunks
    at_edge = (lane < 2) | (lane >= LANES - 2)

    def scatter(b, carry):
        units = [(i, s, g) for i in range(batch) for s in range(SUB) for g in range(groups)]
        depth = 4 * DEPTH
        held = []
        for n in range(len(units) + depth):
            if n < len(units):
                i, s, g = units[n]
                c = b * batch + i
                back = LANES - 2 - (SLOT * s + 2)
                held.append((right(trend_u[c * groups + g], back), right(trend_v[c * groups + g], back)))
            if n >= depth:
                i, s, g = units[n - depth]
                c = b * batch + i
                k = c * SUB + s
                own = pl.ds(k * pitch + PAD + g * SUB, SUB)
                part = pl.ds(k * rows + g * SUB, SUB)
                tr_u, tr_v = held[n - depth]
                u[part, :] = jnp.where(at_edge, um[own, :] + ru[part, :] * tr_u, u[part, :])
                v[part, :] = jnp.where(at_edge, vm[own, :] + rv[part, :] * tr_v, v[part, :])
                if s == SUB - 1 and g == groups - 1:
                    out_copy(c, 0).start()
                    out_copy(c, 1).start()
        return carry

    lax.fori_loop(0, chunks // batch, scatter, 0)
    for c in range(chunks):
        out_copy(c, 0).wait()
        out_copy(c, 1).wait()


def exchange(value, pairs):
    return lax.ppermute(value, ("lat", "lon"), pairs)


def local(u, v, eu, ev, su, sv, fu, fv, seam):
    levels, rows, cols = u.shape
    lats, lons = lax.axis_size("lat"), lax.axis_size("lon")
    assert cols == LANES and levels % SUB == 0 and rows % (4 * SUB) == 0 and lats % 2 == 0 and lons > 1
    pitch = rows + PAD
    groups, chunks = rows // SUB, levels // SUB
    f32 = jnp.float32
    hbm = pl.BlockSpec(memory_space=pltpu.HBM)
    vmem = pl.BlockSpec(memory_space=pltpu.VMEM)
    tile = (SUB, LANES)
    padded = (levels * pitch + PAD, LANES)
    strip = (chunks * pitch + PAD, LANES)
    block = (levels, rows, LANES)
    flat = (levels * rows, LANES)
    line = (6, levels, LANES)
    columns = (chunks * groups,) + tile
    sides = (chunks * groups // 4 * 3,) + tile
    shapes = [padded] * 4 + [flat] * 2 + [strip] * 4 + [line, sides, tile, tile, line]
    outs = [pltpu.VMEM(s, f32) for s in shapes] + [pltpu.VMEM(tile, jnp.int32)]
    packed = pl.pallas_call(
        functools.partial(pack_kernel, levels, rows, lons),
        out_shape=outs,
        in_specs=[hbm] * 9,
        out_specs=[vmem] * len(outs),
        scratch_shapes=[pltpu.VMEM(block, f32)] * 4
        + [pltpu.VMEM(block, jnp.int32)] * 2
        + [pltpu.VMEM((rows, LANES), f32)] * 2
        + [
            pltpu.SMEM(seam.shape, jnp.int32),
            pltpu.SemaphoreType.DMA((chunks, 6)),
            pltpu.SemaphoreType.DMA((3,)),
        ],
        compiler_params=pltpu.CompilerParams(vmem_limit_bytes=16 << 20),
        name="pack",
    )(*(pltpu.with_memory_space_constraint(x, pltpu.HBM) for x in (u, v, eu, ev, su, sv, fu, fv, seam)))
    padded_fields = packed[:4]
    ru, rv = packed[4:6]
    strips = packed[6:10]
    msg_b, msg_x, msg_d, msg_c, msg_a, source = packed[10:]

    def at(k, l):
        return k * lons + l % lons

    every = [(k, l) for k in range(lats) for l in range(lons)]
    to_east = [(at(k, l), at(k, l + 1)) for k, l in every]
    to_west = [(at(k, l), at(k, l - 1)) for k, l in every]
    pair_a = [(at(k, l), at(k ^ 1, l)) for k, l in every]
    pair_c = [(at(k, l), at(k ^ 1, l + 1 if k % 2 else l - 1)) for k, l in every]
    pair_b = []
    pair_d = []
    for k, l in every:
        if k in (0, lats - 1):
            pair_b.append((at(k, l), at(k, l + 1)))
            pair_d.append((at(k, l), at(k, l + 1)))
        elif k % 2:
            pair_b.append((at(k, l), at(k + 1, l)))
            pair_d.append((at(k, l), at(k + 1, l - 1)))
        else:
            pair_b.append((at(k, l), at(k - 1, l)))
            pair_d.append((at(k, l), at(k - 1, l + 1)))
    got_b = exchange(msg_b, pair_b)
    west_x = exchange(msg_x, to_east)
    east_x = west_x if lons == 2 else exchange(msg_x, to_west)
    got_d = exchange(msg_d, pair_d)
    got_c = exchange(msg_c, pair_c)
    got_a = exchange(msg_a, pair_a)
    if lons == 2:
        bands = msg_b
    else:
        bands = lax.all_gather(msg_b, "lon", axis=0, tiled=True)

    points = levels * rows * LANES
    inner = pl.pallas_call(
        functools.partial(inner_kernel, levels, rows),
        out_shape=[pltpu.VMEM(flat, f32)] * 2,
        in_specs=[vmem] * 6,
        out_specs=[vmem] * 2,
        cost_estimate=pl.CostEstimate(flops=60 * points, transcendentals=0, bytes_accessed=32 * points),
        compiler_params=pltpu.CompilerParams(vmem_limit_bytes=16 << 20),
        name="inner",
    )(*padded_fields, ru, rv)

    result = jax.ShapeDtypeStruct(flat, f32)
    done = pl.pallas_call(
        functools.partial(edge_kernel, levels, rows, lons, lats),
        out_shape=[pltpu.VMEM(padded, f32)] * 4 + [pltpu.VMEM(strip, f32)] * 4 + [pltpu.VMEM(flat, f32)] * 2 + [result] * 2,
        in_specs=[vmem] * 20,
        out_specs=[vmem] * 10 + [hbm] * 2,
        input_output_aliases={n: n for n in range(10)},
        scratch_shapes=[
            pltpu.VMEM(line, f32),
            pltpu.VMEM(line, f32),
            pltpu.VMEM((2,) + tile, f32),
            pltpu.VMEM(columns, f32),
            pltpu.VMEM(columns, f32),
            pltpu.SemaphoreType.DMA((chunks, 2)),
        ],
        compiler_params=pltpu.CompilerParams(vmem_limit_bytes=16 << 20),
        name="edge",
    )(*padded_fields, *strips, *inner, ru, rv, got_b, west_x, east_x, got_d, got_c, got_a, bands, source)
    return done[10].reshape(block), done[11].reshape(block)


def solution(mesh):
    tile = P(None, "lat", "lon")
    return jax.shard_map(
        local,
        mesh=mesh,
        in_specs=(tile,) * 4 + (P("lat", "lon"),) * 2 + (tile,) * 2 + (P(),),
        out_specs=(tile, tile),
        check_vma=False,
    )
```
